256 devices in a mesh: basin: 8 (over z), reach: 32 (over x, y, core).
Axes of the slice: x: 4, y: 4, z: 8, core: 2. Of those that a mesh axis runs over, the one named last changes fastest.
Arguments:
- sensitivity: float32 [16, 1024, 256], P(None, ('basin', 'reach')), may hold values from -6 to 6
- inverse: float32 [1024, 256, 256], P(('basin', 'reach')), may hold values from -0.375 to 0.375
- spread: float32 [1024, 256], P(('basin', 'reach')), may hold values from -3 to 3
- gather_weight: float32 [1024, 256], P(('basin', 'reach')), may hold values from -0.0234375 to 0.0234375
- retain: float32 [1024], P(('basin', 'reach')), may hold values from 0.9980469 to 1
- storage: float32 [1024, 256], P(('basin', 'reach')), may hold values from 0.2 to 0.6
- conf_source: int32 [256, 32, 64], P(('basin', 'reach')), may hold values from 0 to 1023
- conf_target: int32 [256, 32, 64], P(('basin', 'reach')), may hold values from 0 to 1023
- conf_weight: float32 [256, 32, 64], P(('basin', 'reach')), may hold values from 0.1 to 0.4
Outputs:
- adjoint: float32 [16, 1024, 256], P(None, ('basin', 'reach'))
The draws below stay inside these ranges and needn't reach their ends.
All inputs are finite; a program needn't handle non-finite values.
Results may differ from the reference program's by a relative error of at most 0.00019.
Values sent between devices are 32-bit elements; how exact they have to be, the bound alone decides.
A program may use at most 64 MiB of HBM per device.

```python
import jax
import jax.numpy as jnp
from jax import lax

R = 256
NB = 4
F = 64
STEPS = 16
PEERS = 32
DEV_COUNT = 256
BLOCKS = 1024


def touch_ends(drawn, own_key, least, top_value):
    spot = [jax.random.randint(jax.random.fold_in(own_key, axis), (), 0, length) for axis, length in enumerate(drawn.shape)]
    longest = drawn.shape.index(max(drawn.shape))
    next_to = spot[:longest] + [(spot[longest] + 1) % drawn.shape[longest]] + spot[longest + 1:]
    return drawn.at[tuple(spot)].set(least).at[tuple(next_to)].set(top_value)


def block_scale(stream_key, shape, split, smallest, top_value):
    factor_of = 1.0
    for position, parts in split:
        draws = jax.random.uniform(jax.random.fold_in(jax.random.fold_in(stream_key, 6), position), (parts,), jnp.float32, smallest / len(split), top_value / len(split))
        factor_of = factor_of * jnp.repeat(jnp.exp(draws), shape[position] // parts).reshape((-1,) + (1,) * (len(shape) - 1 - position))
    return factor_of


def centred(stream_key, extent, scale, most, split=(), held_as=jnp.bfloat16):
    drawn = jax.random.normal(stream_key, extent, jnp.float32) * scale
    if len(split) > 0:
        drawn = block_scale(stream_key, extent, split, -0.22, 0.18) * drawn
    return jnp.clip(drawn, min=-most, max=most).astype(held_as)


def setup_inputs(seed: int = 0) -> dict:
    keys = jax.random.split(jax.random.key(seed), 10)
    sensitivity = centred(keys[0], (STEPS, BLOCKS, R), 1.0, 6.0, ((1, 256),), jnp.float32)
    inverse = centred(keys[1], (BLOCKS, R, R), R ** -0.5, 0.375, ((0, 256),), jnp.float32)
    spread = centred(keys[2], (BLOCKS, R), 0.5, 3.0, ((0, 256),), jnp.float32)
    gather_weight = centred(keys[3], (BLOCKS, R), (R * BLOCKS // 4) ** -0.5, 0.0234375, ((0, 256),), jnp.float32)
    retain = jnp.clip(0.9980469 + 0.001953125 * jax.random.uniform(keys[4], (BLOCKS,), jnp.float32) ** block_scale(keys[4], (BLOCKS,), ((0, 256),), -0.2, 0.2), 0.9980469, 1.0)
    storage = jnp.clip(0.2 + 0.400000021 * jax.random.uniform(keys[5], (BLOCKS, R), jnp.float32) ** block_scale(keys[5], (BLOCKS, R), ((0, 256),), -0.2, 0.2), 0.2, 0.6)
    conf_source = touch_ends(jax.random.randint(keys[6], (DEV_COUNT, PEERS, F), 0, NB * R), jax.random.fold_in(keys[6], 1), 0, (NB * R) - 1).astype(jnp.int32)
    conf_target = touch_ends(jax.random.randint(keys[7], (DEV_COUNT, PEERS, F), 0, NB * R), jax.random.fold_in(keys[7], 1), 0, (NB * R) - 1).astype(jnp.int32)
    conf_weight = jnp.clip(0.1 + 0.3 * jax.random.uniform(keys[8], (DEV_COUNT, PEERS, F), jnp.float32) ** block_scale(keys[8], (DEV_COUNT, PEERS, F), ((0, 256),), -0.2, 0.2), 0.1, 0.4)
    return {"sensitivity": sensitivity, "inverse": inverse, "spread": spread, "gather_weight": gather_weight, "retain": retain, "storage": storage, "conf_source": conf_source, "conf_target": conf_target, "conf_weight": conf_weight}


def reference(sensitivity, inverse, spread, gather_weight, retain, storage, conf_source, conf_target, conf_weight):
    rows = NB * R
    group = (jnp.arange(DEV_COUNT, dtype=jnp.int32) // PEERS) * PEERS
    src_dev = jnp.broadcast_to(group[:, None, None] + jnp.arange(PEERS, dtype=jnp.int32)[None, :, None], conf_source.shape)
    dev_ids = jnp.broadcast_to(jnp.arange(DEV_COUNT, dtype=jnp.int32)[:, None, None], conf_target.shape)

    def step(later, forcing_now):
        flat = later.reshape(DEV_COUNT, rows)
        values = flat[src_dev, conf_source] * conf_weight
        fan = jnp.zeros((DEV_COUNT, rows), jnp.float32).at[dev_ids, conf_target].add(values)
        forcing = forcing_now + storage * later + fan.reshape(BLOCKS, R)
        local = jnp.einsum("bij,bi->bj", inverse, forcing, precision=lax.Precision.HIGHEST)
        feed = jnp.sum(gather_weight * local, axis=1)

        def link(stem, pair):
            keep, term = pair
            return keep * stem + term, stem

        _, stem_next = lax.scan(link, jnp.zeros((), jnp.float32), (retain, feed), reverse=True)
        adjoint = local + spread * stem_next[:, None]
        return adjoint, adjoint

    _, adjoint = lax.scan(step, jnp.zeros((BLOCKS, R), jnp.float32), sensitivity, reverse=True)
    return adjoint
```

```python
import functools

import jax
import jax.numpy as jnp
from jax import lax
from jax.experimental import pallas as pl
from jax.experimental.pallas import tpu as pltpu
from jax.sharding import PartitionSpec as P

LANES = 128
MESH = pl.DeviceIdType.MESH


def lane_take(row, index):
    return jnp.take_along_axis(jnp.broadcast_to(row, index.shape), index, axis=1)


def split_halves(x):
    return jnp.concatenate([x[:, :LANES], x[:, LANES:]], axis=0)


def place(j):
    return ((j >> 7) & 1) * 4 + (j >> 8), j & 127


def kernel(
    basins, peers, steps,
    sens_ref, inv_ref, spread_ref, gather_ref, retain_ref, storage_ref,
    source_ref, target_ref, weight_ref,
    out_ref,
    send_buf, recv_buf, once_send, once_recv, z_send, z_recv,
    coef_ref, hot_ref, mask_ref,
    send_sem, recv_sem, once_send_sem, once_recv_sem, z_send_sem, z_recv_sem,
):
    g = lax.axis_index("basin")
    me = lax.axis_index("reach")
    half = peers // 2
    f32 = jnp.float32

    if peers == 32:
        x, y, c = me // 8, (me // 2) % 4, me % 2
        hop = (0, 1, 2, 1)
        order = sorted(
            ((dx, dy, dc) for dx in range(4) for dy in range(4) for dc in range(2)),
            key=lambda d: -(hop[d[0]] + hop[d[1]]) * 2 - d[2],
        )
        others = [
            (((x + dx) % 4) * 4 + (y + dy) % 4) * 2 + (c + dc) % 2
            for dx, dy, dc in order
            if (dx, dy, dc) != (0, 0, 0)
        ]
    else:
        others = [(me + d) % peers for d in range(1, peers)]

    barrier = pltpu.get_barrier_semaphore()
    for p in others:
        pl.semaphore_signal(barrier, inc=1, device_id={"reach": p}, device_id_type=MESH)

    @pl.when(g > 0)
    def _():
        pl.semaphore_signal(barrier, inc=1, device_id={"basin": g - 1}, device_id_type=MESH)

    @pl.when(g < basins - 1)
    def _():
        pl.semaphore_signal(barrier, inc=1, device_id={"basin": g + 1}, device_id_type=MESH)

    lane = lax.broadcasted_iota(jnp.int32, (peers, LANES), 1)
    row = lax.broadcasted_iota(jnp.int32, (peers, LANES), 0)
    low = lane < 64
    low_half = low[:half]
    lane8 = lax.broadcasted_iota(jnp.int32, (8, LANES), 1)
    row8 = lax.broadcasted_iota(jnp.int32, (8, LANES), 0)
    block8 = row8 % 4

    r0, r1, r2, r3 = (retain_ref[i] for i in range(4))
    slope_me = r0 * r1 * r2 * r3

    first = jnp.concatenate(
        [source_ref[0].astype(f32), jnp.full((peers, 64), slope_me, f32)], axis=1
    )
    once_send[0] = first.reshape(peers, 1, LANES)
    once_recv[0, pl.ds(me, 1)] = once_send[0, pl.ds(me, 1)]

    neighbours = (g > 0).astype(jnp.int32) + (g < basins - 1).astype(jnp.int32)
    pl.semaphore_wait(barrier, peers - 1 + neighbours)

    def to_all(src, dst, s_sem, r_sem):
        for p in others:
            pltpu.make_async_remote_copy(
                src_ref=src.at[pl.ds(p, 1)], dst_ref=dst.at[pl.ds(me, 1)],
                send_sem=s_sem, recv_sem=r_sem,
                device_id={"reach": p}, device_id_type=MESH,
            ).start()

    def all_done(buf, sem):
        part = buf.at[pl.ds(0, peers - 1)]
        pltpu.make_async_copy(part, part, sem).wait()

    to_all(once_send.at[0], once_recv.at[0], once_send_sem.at[0], once_recv_sem.at[0])

    @pl.when(g == basins - 1)
    def _():
        z_recv[...] = jnp.zeros_like(z_recv)

    spread = split_halves(spread_ref[...])
    storage = split_halves(storage_ref[...])
    keep = [
        jnp.where(block8 == 0, a, jnp.where(block8 == 1, b, jnp.where(block8 == 2, d, e)))
        for a, b, d, e in (
            (1.0, r0, r0 * r1, r0 * r1 * r2),
            (1.0, 1.0, 1.0, 0.0),
            (r1, r2, 0.0, 0.0),
            (r1 * r2, 0.0, 0.0, 0.0),
            (r1 * r2 * r3, r2 * r3, r3, 1.0),
        )
    ]
    spread_in = spread * keep[4]

    target = jnp.concatenate([target_ref[0, :half], target_ref[0, half:]], axis=1)
    weight = jnp.concatenate([weight_ref[0, :half], weight_ref[0, half:]], axis=1)
    t_row, t_lane = place(target)
    sub = lax.broadcasted_iota(jnp.int32, (LANES, LANES), 0)
    for q in range(half):
        mask_ref[q] = jnp.where(row8 == t_row[q : q + 1], weight[q : q + 1], 0.0)
        hot = jnp.where(sub == t_lane[q : q + 1], 1.0, 0.0)
        hot_ref[q * LANES : (q + 1) * LANES, :] = hot.T.astype(jnp.bfloat16)

    feed_row = split_halves(
        jnp.concatenate(
            [
                lax.dot_general(
                    gather_ref[b : b + 1], inv_ref[b], (((1,), (1,)), ((), ())),
                    precision=lax.Precision.HIGHEST, preferred_element_type=f32,
                )
                for b in range(4)
            ],
            axis=0,
        )
    )

    all_done(once_recv.at[0], once_recv_sem.at[0])
    got = once_recv[0].reshape(peers, LANES)
    asked_row, asked_lane = place(jnp.where(low, got, 0.0).astype(jnp.int32))
    slope = jnp.where(low, pltpu.roll(got, 64, 1), got)

    rest, d = slope, 1
    level = 0
    while d < peers:
        coef_ref[level] = jnp.where(row + d < peers, rest, 0.0)
        rest = rest * jnp.where(row + d < peers, pltpu.roll(rest, peers - d, 0), 1.0)
        d, level = 2 * d, level + 1
    levels = level
    past = jnp.where(row < peers - 1, pltpu.roll(rest, peers - 1, 0), 1.0)
    whole = rest[0:1]

    def picked(x):
        out = jnp.zeros((peers, LANES), f32)
        for r in range(8):
            out = jnp.where(asked_row == r, lane_take(x[r : r + 1], asked_lane), out)
        return out

    once_send[1] = picked(spread_in).reshape(peers, 1, LANES)
    once_recv[1, pl.ds(me, 1)] = once_send[1, pl.ds(me, 1)]

    column = lax.broadcasted_iota(jnp.int32, (LANES, LANES), 0)

    def advance(k, forcing):
        part = jnp.broadcast_to(
            jnp.sum(forcing * feed_row, axis=1, keepdims=True), (8, LANES)
        )
        feed = part + pltpu.roll(part, 4, 0)
        offset = jnp.sum(keep[0] * part, axis=0, keepdims=True)
        within = (
            keep[1] * pltpu.roll(feed, 7, 0)
            + keep[2] * pltpu.roll(feed, 6, 0)
            + keep[3] * pltpu.roll(feed, 5, 0)
        )
        sums = []
        for b in range(4):
            total = jnp.zeros((8, 2 * LANES), f32)
            for h in range(2):
                col = lane_take(forcing[h * 4 + b : h * 4 + b + 1], column)
                col = jnp.concatenate([col, col], axis=1)
                block = inv_ref[b, h * LANES : (h + 1) * LANES, :]
                total = total + jnp.sum((col * block).reshape(16, 8, 2 * LANES), axis=0)
            sums.append(jnp.sum(total, axis=0, keepdims=True))
        local = split_halves(jnp.concatenate(sums, axis=0))
        partial = local + spread * within
        message = jnp.where(low, picked(partial), jnp.broadcast_to(offset, (peers, LANES)))
        send_buf[k] = message.reshape(peers, 1, LANES)
        to_all(send_buf.at[k], recv_buf.at[k], send_sem.at[k], recv_sem.at[k])
        recv_buf[k, pl.ds(me, 1)] = send_buf[k, pl.ds(me, 1)]
        return partial

    def arrive(k, partial):
        all_done(recv_buf.at[k], recv_sem.at[k])
        rows = recv_buf[k].reshape(peers, LANES)
        turned = pltpu.roll(rows, 64, 1)
        stem = jnp.where(low, turned, rows)
        for level in range(levels):
            stem = stem + coef_ref[level] * pltpu.roll(stem, peers - 2**level, 0)

        @pl.when(g < basins - 1)
        def _():
            here = z_recv.at[k]
            pltpu.make_async_copy(here, here, z_recv_sem.at[k]).wait()

        outer = z_recv[k]

        @pl.when(g > 0)
        def _():
            z_send[k] = stem[0:1] + whole * outer
            pltpu.make_async_remote_copy(
                src_ref=z_send.at[k], dst_ref=z_recv.at[k],
                send_sem=z_send_sem.at[k], recv_sem=z_recv_sem.at[k],
                device_id={"basin": g - 1}, device_id_type=MESH,
            ).start()

        entering = jnp.where(row < peers - 1, pltpu.roll(stem, peers - 1, 0), 0.0)
        entering = entering + past * outer
        own = jnp.sum(jnp.where(row == me, entering, 0.0), axis=0, keepdims=True)
        adjoint = partial + spread_in * own
        t = steps - 1 - k
        out_ref[t, :, 0:LANES] = adjoint[0:4]
        out_ref[t, :, LANES : 2 * LANES] = adjoint[4:8]
        return rows, turned, entering, adjoint

    partial = advance(0, split_halves(sens_ref[steps - 1]))
    to_all(once_send.at[1], once_recv.at[1], once_send_sem.at[1], once_recv_sem.at[1])
    all_done(once_recv.at[1], once_recv_sem.at[1])
    got = once_recv[1].reshape(peers, LANES)
    spread_at = jnp.where(low_half, got[:half], pltpu.roll(got[half:], 64, 1))

    def body(k, partial):
        rows, turned, entering, adjoint = arrive(k - 1, partial)
        values = jnp.where(low_half, rows[:half], turned[half:])
        stems = jnp.where(low_half, entering[:half], entering[half:])
        values = values + spread_at * stems
        fan = jnp.zeros((16, LANES), f32)
        lines = []
        for q in range(half):
            line = values[q : q + 1] * mask_ref[q]
            coarse = line.astype(jnp.bfloat16).astype(f32)
            lines.append(jnp.concatenate([coarse, line - coarse], axis=0).astype(jnp.bfloat16))
        fan = jnp.dot(
            jnp.concatenate(lines, axis=1), hot_ref[...], preferred_element_type=f32
        )
        forcing = (
            split_halves(sens_ref[steps - 1 - k]) + storage * adjoint + (fan[0:8] + fan[8:16])
        )
        return advance(k, forcing)

    partial = lax.fori_loop(1, steps, body, partial)
    arrive(steps - 1, partial)

    for i in range(2):
        all_done(once_send.at[i], once_send_sem.at[i])

    def drain(k, carry):
        all_done(send_buf.at[k], send_sem.at[k])

        @pl.when(g > 0)
        def _():
            here = z_send.at[k]
            pltpu.make_async_copy(here, here, z_send_sem.at[k]).wait()

        return carry

    lax.fori_loop(0, steps, drain, 0)


def solution(mesh):
    basins, peers = mesh.shape["basin"], mesh.shape["reach"]
    both = ("basin", "reach")

    def on_device(*args):
        steps, blocks, reaches = args[0].shape
        vmem = pl.BlockSpec(memory_space=pltpu.VMEM)
        smem = pl.BlockSpec(memory_space=pltpu.SMEM)
        levels = max(1, (peers - 1).bit_length())
        dma = pltpu.SemaphoreType.DMA
        return pl.pallas_call(
            functools.partial(kernel, basins, peers, steps),
            out_shape=jax.ShapeDtypeStruct((steps, blocks, reaches), jnp.float32),
            in_specs=[vmem] * 4 + [smem] + [vmem] * 4,
            out_specs=vmem,
            scratch_shapes=[
                pltpu.VMEM((steps, peers, 1, LANES), jnp.float32),
                pltpu.VMEM((steps, peers, 1, LANES), jnp.float32),
                pltpu.VMEM((2, peers, 1, LANES), jnp.float32),
                pltpu.VMEM((2, peers, 1, LANES), jnp.float32),
                pltpu.VMEM((steps, 1, LANES), jnp.float32),
                pltpu.VMEM((steps, 1, LANES), jnp.float32),
                pltpu.VMEM((levels, peers, LANES), jnp.float32),
                pltpu.VMEM((peers // 2 * LANES, LANES), jnp.bfloat16),
                pltpu.VMEM((peers // 2, 8, LANES), jnp.float32),
                dma((steps,)), dma((steps,)), dma((2,)), dma((2,)),
                dma((steps,)), dma((steps,)),
            ],
            compiler_params=pltpu.CompilerParams(collective_id=0, has_side_effects=True),
        )(*args)

    two, three = P(both, None), P(both, None, None)
    return jax.shard_map(
        on_device,
        mesh=mesh,
        in_specs=(P(None, both, None), three, two, two, P(both), two, three, three, three),
        out_specs=P(None, both, None),
        check_vma=False,
    )
```
